8 devices in a mesh: dp: 1 (over z), tp: 8 (over y, x, core).
Axes of the slice: x: 2, y: 2, z: 1, core: 2. Of those that a mesh axis runs over, the one named last changes fastest.
Arguments:
- x_a: bfloat16 [4096, 4096], P(('dp', 'tp'))
- x_b: bfloat16 [4096, 4096], P(('dp', 'tp'))
- labels_a: int32 [4096], P(('dp', 'tp'))
- labels_b: int32 [4096], P(('dp', 'tp'))
- w_head: bfloat16 [4096, 32768], P(None, 'tp')
Outputs:
- output 1: float32 [2], P('dp')
- output 2: bfloat16 [4096, 32768], P('dp', 'tp')
- output 3: bfloat16 [4096, 4096], P(('dp', 'tp'))
- output 4: bfloat16 [4096, 4096], P(('dp', 'tp'))
All inputs are finite; a program needn't handle non-finite values.
Results may differ from the reference program's by a relative error of at most 0.001.
Values are sent between devices in bfloat16 or wider.
A program may use at most 1 GiB of HBM per device.

```python
import math
import jax
import jax.numpy as jnp
from jax import lax

TOKENS = 4096
HIDDEN = 4096
VOCAB = 32768
VOCAB_SPLIT = 8


def draw_labels(label_key):
    value_key, first_key, gap_key = jax.random.split(label_key, 3)
    label_ids = jax.random.randint(value_key, (TOKENS,), 0, VOCAB, jnp.int32)
    first_pos = jax.random.randint(first_key, (), 0, TOKENS, jnp.int32)
    second_pos = (first_pos + jax.random.randint(gap_key, (), 1, TOKENS, jnp.int32)) % TOKENS
    return label_ids.at[first_pos].set(0).at[second_pos].set(VOCAB - 1)


def setup_inputs(seed: int = 0, part: int = 0) -> dict:
    part_key = jax.random.fold_in(jax.random.key(seed), part)
    key_xa, key_xb, key_la, key_lb = jax.random.split(part_key, 4)
    x_a = jax.random.normal(key_xa, (TOKENS, HIDDEN), jnp.float32).astype(jnp.bfloat16)
    x_b = jax.random.normal(key_xb, (TOKENS, HIDDEN), jnp.float32).astype(jnp.bfloat16)
    w_scale = 2.5 / math.sqrt(HIDDEN)
    w_head = (jax.random.normal(jax.random.key(seed + 1), (HIDDEN, VOCAB), jnp.float32) * w_scale).astype(jnp.bfloat16)
    return {"x_a": x_a, "x_b": x_b, "labels_a": draw_labels(key_la), "labels_b": draw_labels(key_lb), "w_head": w_head}


def reference(x_a, x_b, labels_a, labels_b, w_head):
    shard_cols = VOCAB // VOCAB_SPLIT
    w_blocks = w_head.reshape(HIDDEN, VOCAB_SPLIT, shard_cols).transpose(1, 0, 2)
    offsets = jnp.arange(VOCAB_SPLIT, dtype=jnp.int32) * shard_cols
    x_flat = jnp.concatenate([x_a, x_b], axis=0)
    label_flat = jnp.concatenate([labels_a, labels_b], axis=0)
    col_ids = jnp.arange(shard_cols, dtype=jnp.int32)[None, :]

    def block_stats(block_args):
        w_block, offset = block_args
        logits = jnp.dot(x_flat, w_block, preferred_element_type=jnp.float32)
        block_max = jnp.max(logits, axis=1)
        block_sum = jnp.sum(jnp.exp(logits - block_max[:, None]), axis=1)
        label_hit = col_ids == (label_flat - offset)[:, None]
        block_target = jnp.sum(jnp.where(label_hit, logits, 0.0), axis=1)
        return block_max, block_sum, block_target

    all_max, all_sum, all_target = lax.map(block_stats, (w_blocks, offsets))
    row_max = jnp.max(all_max, axis=0)
    row_sum = jnp.sum(all_sum * jnp.exp(all_max - row_max[None, :]), axis=0)
    target = jnp.sum(all_target, axis=0)
    loss_tok = row_max + jnp.log(row_sum) - target
    losses = jnp.stack([jnp.mean(loss_tok[:TOKENS]), jnp.mean(loss_tok[TOKENS:])])

    def block_grad(dx_acc, block_args):
        w_block, offset = block_args
        logits = jnp.dot(x_flat, w_block, preferred_element_type=jnp.float32)
        label_hit = col_ids == (label_flat - offset)[:, None]
        probs = jnp.exp(logits - row_max[:, None]) / row_sum[:, None]
        grad_logits = ((probs - label_hit.astype(jnp.float32)) / TOKENS).astype(jnp.bfloat16)
        grad_block = jnp.dot(x_flat.T, grad_logits, preferred_element_type=jnp.float32).astype(jnp.bfloat16)
        dx_acc = dx_acc + jnp.dot(grad_logits, w_block.T, preferred_element_type=jnp.float32)
        return dx_acc, grad_block

    dx_init = jnp.zeros((2 * TOKENS, HIDDEN), jnp.float32)
    dx_sum, grad_blocks = lax.scan(block_grad, dx_init, (w_blocks, offsets))
    grad_w = grad_blocks.transpose(1, 0, 2).reshape(HIDDEN, VOCAB)
    grad_x = dx_sum.astype(jnp.bfloat16)
    return losses, grad_w, grad_x[:TOKENS], grad_x[TOKENS:]
```

```python
import functools

import jax
import jax.numpy as jnp
from jax import lax
from jax.experimental import pallas as pl
from jax.experimental.pallas import tpu as pltpu
from jax.sharding import PartitionSpec as P

PIECES = ((0, 128), (0, 128), (0, 256), (1, 256), (1, 256))
LANES = 128


def logits_kernel(cols, x_ref, w_ref, lab_ref, z_ref, m_ref, s_ref, t_ref, m_acc, s_acc, t_acc):
    v = pl.program_id(0)
    rows, tile = x_ref.shape[0], 512

    @pl.when(v == 0)
    def _():
        m_acc[...] = jnp.full_like(m_acc, -jnp.inf)
        s_acc[...] = jnp.zeros_like(s_acc)
        t_acc[...] = jnp.zeros_like(t_acc)

    def fold(start, count):
        sl = pl.ds(start, count)
        lab = lab_ref[sl, :] - v * cols
        parts = [z_ref[sl, k:k + LANES] for k in range(0, cols, LANES)]
        m_old = m_acc[sl, :]
        m_new = functools.reduce(jnp.maximum, parts, m_old)
        total = s_acc[sl, :] * jnp.exp(m_old - m_new)
        target = t_acc[sl, :]
        lane = lax.broadcasted_iota(jnp.int32, (count, LANES), 1)
        for k, part in enumerate(parts):
            total = total + jnp.exp(part - m_new)
            target = target + jnp.where(lane == lab - k * LANES, part, 0.0)
        m_acc[sl, :], s_acc[sl, :], t_acc[sl, :] = m_new, total, target

    for r in range(0, rows + tile, tile):
        if r > 0:
            for q in range(r - tile, r, 64):
                fold(q, 64)
        if r < rows:
            z_ref[r:r + tile, :] = jnp.dot(x_ref[r:r + tile, :], w_ref[...], preferred_element_type=jnp.float32)

    @pl.when(v == pl.num_programs(0) - 1)
    def _():
        m = jnp.max(m_acc[...], axis=1, keepdims=True)
        s = jnp.sum(s_acc[...] * jnp.exp(m_acc[...] - m), axis=1, keepdims=True)
        t = jnp.sum(t_acc[...], axis=1, keepdims=True)
        m_ref[...] = jnp.broadcast_to(m, m_ref.shape)
        s_ref[...] = jnp.broadcast_to(s, s_ref.shape)
        t_ref[...] = jnp.broadcast_to(t, t_ref.shape)


def logits_call(x, w, lab, cols=512):
    rows, hidden = x.shape
    vocab = w.shape[1]
    stat = jax.ShapeDtypeStruct((rows, LANES), jnp.float32)
    stat_spec = pl.BlockSpec((rows, LANES), lambda v: (0, 0))
    return pl.pallas_call(
        functools.partial(logits_kernel, cols), name="logits",
        grid=(vocab // cols,),
        in_specs=[pl.BlockSpec((rows, hidden), lambda v: (0, 0)), pl.BlockSpec((hidden, cols), lambda v: (0, v)), pl.BlockSpec((rows, 1), lambda v: (0, 0))],
        out_specs=[pl.BlockSpec((rows, cols), lambda v: (0, v)), stat_spec, stat_spec, stat_spec],
        out_shape=[jax.ShapeDtypeStruct((rows, vocab), jnp.float32), stat, stat, stat],
        scratch_shapes=[pltpu.VMEM((rows, LANES), jnp.float32)] * 3,
        compiler_params=pltpu.CompilerParams(vmem_limit_bytes=63 << 20, dimension_semantics=("arbitrary",)),
        cost_estimate=pl.CostEstimate(flops=2 * rows * hidden * vocab, bytes_accessed=(rows + vocab) * hidden * 2 + rows * vocab * 4, transcendentals=rows * vocab),
    )(x, w, lab)


def wgrad_kernel(count, *refs):
    total = None
    for x_ref, g_ref in zip(refs[:count], refs[count:2 * count]):
        part = lax.dot_general(x_ref[...], g_ref[...], (((0,), (0,)), ((), ())), preferred_element_type=jnp.float32)
        total = part if total is None else total + part
    refs[-1][...] = total.astype(refs[-1].dtype)


def wgrad_call(xs, gs, bh=512, bv=1024):
    hidden, vocab, rows = xs[0].shape[1], gs[0].shape[1], sum(x.shape[0] for x in xs)
    return pl.pallas_call(
        functools.partial(wgrad_kernel, len(xs)), name="wgrad",
        grid=(vocab // bv, hidden // bh),
        in_specs=[pl.BlockSpec((x.shape[0], bh), lambda v, h: (0, h)) for x in xs] + [pl.BlockSpec((g.shape[0], bv), lambda v, h: (0, v)) for g in gs],
        out_specs=pl.BlockSpec((bh, bv), lambda v, h: (h, v)),
        out_shape=jax.ShapeDtypeStruct((hidden, vocab), jnp.bfloat16),
        compiler_params=pltpu.CompilerParams(vmem_limit_bytes=63 << 20, dimension_semantics=("arbitrary", "arbitrary")),
        cost_estimate=pl.CostEstimate(flops=2 * rows * hidden * vocab, bytes_accessed=rows * (hidden + vocab) * 2 + hidden * vocab * 2, transcendentals=0),
    )(*xs, *gs)


def after(value, token):
    return lax.optimization_barrier((value, token))[0]


def solution(mesh):
    n = mesh.shape["tp"]

    def local_step(x_a, x_b, labels_a, labels_b, w):
        tokens = x_a.shape[0] * n
        cols = w.shape[1]
        me = lax.axis_index("tp")
        xs = (x_a, x_b)
        labels = lax.all_gather(jnp.stack([labels_a, labels_b]), "tp", axis=0, tiled=False) - me * cols
        col_ids = lax.broadcasted_iota(jnp.int32, (1, cols), 1)
        starts, fill = [], [0, 0]
        for mb, size in PIECES:
            starts.append(fill[mb])
            fill[mb] += size

        def gather(i, token=None):
            mb, size = PIECES[i]
            x = xs[mb][starts[i]:starts[i] + size]
            x = x if token is None else after(x, token)
            return lax.all_gather(x, "tp", axis=0, tiled=True)

        labs = [labels[:, mb, s0:s0 + size].reshape(-1, 1) for (mb, size), s0 in zip(PIECES, starts)]

        def forward(i, x, token=None):
            x = x if token is None else after(x, token)
            z, m, s, t = logits_call(x, w, labs[i])
            return z, jnp.stack([m[:, 0], s[:, 0], t[:, 0]])

        def combine(parts):
            every = lax.all_gather(jnp.concatenate(parts, axis=1), "tp", axis=0, tiled=False)
            m_all, s_all, t_all = every[:, 0], every[:, 1], every[:, 2]
            m = jnp.max(m_all, axis=0)
            s = jnp.sum(s_all * jnp.exp(m_all - m), axis=0)
            return m, s, jnp.mean(m + jnp.log(s) - jnp.sum(t_all, axis=0))

        def backward(i, z, stat, token):
            z = after(z, token)
            lo, hi = starts[i] * n, (starts[i] + PIECES[i][1]) * n
            m, s = stat[0][lo:hi, None], stat[1][lo:hi, None]
            hit = (col_ids == labs[i]).astype(jnp.float32)
            g = ((jnp.exp(z - m) / s - hit) / tokens).astype(jnp.bfloat16)
            g = lax.optimization_barrier(g)
            part = lax.dot_general(g, w, (((1,), (1,)), ((), ())), preferred_element_type=jnp.float32)
            return g, part, lax.psum_scatter(part, "tp", scatter_dimension=0, tiled=True)

        gx = [gather(i) for i in range(5)]
        z0, st0 = forward(0, gx[0])
        z1, st1 = forward(1, gx[1], z0)
        z2, st2 = forward(2, gx[2], z1)
        stat_a = combine([st0, st1, st2])
        b0 = backward(0, z0, stat_a, z2)
        b1 = backward(1, z1, stat_a, (b0[1], gx[3], gx[4]))
        b2 = backward(2, z2, stat_a, b1[1])
        z3, st3 = forward(3, gx[3], b2[1])
        z4, st4 = forward(4, gx[4], (z3, b0[2]))
        stat_b = combine([st3, st4])
        b3 = backward(3, z3, stat_b, (z4, b1[2]))
        b4 = backward(4, z4, stat_b, b3[1])
        b = [b0, b1, b2, b3, b4]
        grad_w = wgrad_call(gx, [b0[0], b1[0], b2[0], b3[0], after(b4[0], b4[1])])
        dx = [v[2].astype(jnp.bfloat16) for v in b]
        losses = jnp.stack([stat_a[2], stat_b[2]])
        return losses, grad_w, jnp.concatenate(dx[:3]), jnp.concatenate(dx[3:])

    row_spec = P(("dp", "tp"), None)
    label_spec = P(("dp", "tp"))
    return jax.shard_map(local_step, mesh=mesh, in_specs=(row_spec, row_spec, label_spec, label_spec, P(None, "tp")), out_specs=(P("dp"), P("dp", "tp"), row_spec, row_spec), check_vma=False)
```

```python
import functools

import jax
import jax.numpy as jnp
from jax import lax
from jax.experimental import pallas as pl
from jax.experimental.pallas import tpu as pltpu
from jax.sharding import PartitionSpec as P

PIECES = ((0, 192), (0, 192), (0, 128), (1, 256), (1, 256))
LANES = 128


def logits_kernel(cols, x_ref, w_ref, lab_ref, z_ref, st_ref, m_acc, s_acc, t_acc):
    v = pl.program_id(0)
    rows, tile = x_ref.shape[0], 512

    @pl.when(v == 0)
    def _():
        m_acc[...] = jnp.full_like(m_acc, -jnp.inf)
        s_acc[...] = jnp.zeros_like(s_acc)
        t_acc[...] = jnp.zeros_like(t_acc)

    def fold(start, count):
        sl = pl.ds(start, count)
        lab = lab_ref[sl, :] - v * cols
        parts = [z_ref[sl, k:k + LANES] for k in range(0, cols, LANES)]
        m_old = m_acc[sl, :]
        m_new = functools.reduce(jnp.maximum, parts, m_old)
        total = s_acc[sl, :] * jnp.exp(m_old - m_new)
        target = t_acc[sl, :]
        lane = lax.broadcasted_iota(jnp.int32, (count, LANES), 1)
        for k, part in enumerate(parts):
            total = total + jnp.exp(part - m_new)
            target = target + jnp.where(lane == lab - k * LANES, part, 0.0)
        m_acc[sl, :], s_acc[sl, :], t_acc[sl, :] = m_new, total, target

    for r in range(0, rows + tile, tile):
        if r > 0:
            for q in range(r - tile, r, 64):
                fold(q, 64)
        if r < rows:
            z_ref[r:r + tile, :] = jnp.dot(x_ref[r:r + tile, :], w_ref[...], preferred_element_type=jnp.float32)

    @pl.when(v == pl.num_programs(0) - 1)
    def _():
        m = jnp.max(m_acc[...], axis=1, keepdims=True)
        s = jnp.sum(s_acc[...] * jnp.exp(m_acc[...] - m), axis=1, keepdims=True)
        t = jnp.sum(t_acc[...], axis=1, keepdims=True)
        lane = lax.broadcasted_iota(jnp.int32, st_ref.shape, 1)
        st_ref[...] = jnp.where(lane == 0, m, jnp.where(lane == 1, s, t))


def logits_call(x, w, lab, cols=512):
    rows, hidden = x.shape
    vocab = w.shape[1]
    stat = jax.ShapeDtypeStruct((rows, LANES), jnp.float32)
    stat_spec = pl.BlockSpec((rows, LANES), lambda v: (0, 0))
    return pl.pallas_call(
        functools.partial(logits_kernel, cols), name="logits",
        grid=(vocab // cols,),
        in_specs=[pl.BlockSpec((rows, hidden), lambda v: (0, 0)), pl.BlockSpec((hidden, cols), lambda v: (0, v)), pl.BlockSpec((rows, 1), lambda v: (0, 0))],
        out_specs=[pl.BlockSpec((rows, cols), lambda v: (0, v)), stat_spec],
        out_shape=[jax.ShapeDtypeStruct((rows, vocab), jnp.float32), stat],
        scratch_shapes=[pltpu.VMEM((rows, LANES), jnp.float32)] * 3,
        compiler_params=pltpu.CompilerParams(vmem_limit_bytes=63 << 20, dimension_semantics=("arbitrary",)),
        cost_estimate=pl.CostEstimate(flops=2 * rows * hidden * vocab, bytes_accessed=(rows + vocab) * hidden * 2 + rows * vocab * 4, transcendentals=rows * vocab),
    )(x, w, lab)


def wgrad_kernel(count, *refs):
    total = None
    for x_ref, g_ref in zip(refs[:count], refs[count:2 * count]):
        part = lax.dot_general(x_ref[...], g_ref[...], (((0,), (0,)), ((), ())), preferred_element_type=jnp.float32)
        total = part if total is None else total + part
    refs[-1][...] = total.astype(refs[-1].dtype)


def wgrad_call(xs, gs, bh=512, bv=1024):
    hidden, vocab, rows = xs[0].shape[1], gs[0].shape[1], sum(x.shape[0] for x in xs)
    return pl.pallas_call(
        functools.partial(wgrad_kernel, len(xs)), name="wgrad",
        grid=(vocab // bv, hidden // bh),
        in_specs=[pl.BlockSpec((x.shape[0], bh), lambda v, h: (0, h)) for x in xs] + [pl.BlockSpec((g.shape[0], bv), lambda v, h: (0, v)) for g in gs],
        out_specs=pl.BlockSpec((bh, bv), lambda v, h: (h, v)),
        out_shape=jax.ShapeDtypeStruct((hidden, vocab), jnp.bfloat16),
        compiler_params=pltpu.CompilerParams(vmem_limit_bytes=63 << 20, dimension_semantics=("arbitrary", "arbitrary")),
        cost_estimate=pl.CostEstimate(flops=2 * rows * hidden * vocab, bytes_accessed=rows * (hidden + vocab) * 2 + hidden * vocab * 2, transcendentals=0),
    )(*xs, *gs)


def after(value, token):
    return lax.optimization_barrier((value, token))[0]


def solution(mesh):
    n = mesh.shape["tp"]

    def local_step(x_a, x_b, labels_a, labels_b, w):
        tokens = x_a.shape[0] * n
        cols = w.shape[1]
        me = lax.axis_index("tp")
        xs = (x_a, x_b)
        labels = lax.all_gather(jnp.stack([labels_a, labels_b]), "tp", axis=0, tiled=False) - me * cols
        col_ids = lax.broadcasted_iota(jnp.int32, (1, cols), 1)
        starts, fill = [], [0, 0]
        for mb, size in PIECES:
            starts.append(fill[mb])
            fill[mb] += size

        def gather(i, token=None):
            mb, size = PIECES[i]
            x = xs[mb][starts[i]:starts[i] + size]
            x = x if token is None else after(x, token)
            return lax.all_gather(x, "tp", axis=0, tiled=True)

        labs = [labels[:, mb, s0:s0 + size].reshape(-1, 1) for (mb, size), s0 in zip(PIECES, starts)]

        def forward(i, x, token=None):
            x = x if token is None else after(x, token)
            z, st = logits_call(x, w, labs[i])
            return z, st[:, :3].T

        def combine(parts):
            every = lax.all_gather(jnp.concatenate(parts, axis=1), "tp", axis=0, tiled=False)
            m_all, s_all, t_all = every[:, 0], every[:, 1], every[:, 2]
            m = jnp.max(m_all, axis=0)
            s = jnp.sum(s_all * jnp.exp(m_all - m), axis=0)
            return m, s, jnp.mean(m + jnp.log(s) - jnp.sum(t_all, axis=0))

        def backward(i, z, stat, token):
            z = after(z, token)
            lo, hi = starts[i] * n, (starts[i] + PIECES[i][1]) * n
            m, s = stat[0][lo:hi, None], stat[1][lo:hi, None]
            hit = (col_ids == labs[i]).astype(jnp.float32)
            g = ((jnp.exp(z - m) / s - hit) / tokens).astype(jnp.bfloat16)
            g = lax.optimization_barrier(g)
            part = lax.dot_general(g, w, (((1,), (1,)), ((), ())), preferred_element_type=jnp.float32)
            return g, part, lax.psum_scatter(part, "tp", scatter_dimension=0, tiled=True)

        gx = [gather(i) for i in range(5)]
        z0, st0 = forward(0, gx[0])
        z1, st1 = forward(1, gx[1], z0)
        z2, st2 = forward(2, gx[2], z1)
        stat_a = combine([st0, st1, st2])
        b0 = backward(0, z0, stat_a, z2)
        b1 = backward(1, z1, stat_a, b0[1])
        b2 = backward(2, z2, stat_a, (b1[1], gx[3], gx[4]))
        z3, st3 = forward(3, gx[3], b2[1])
        z4, st4 = forward(4, gx[4], (z3, b0[2]))
        stat_b = combine([st3, st4])
        b3 = backward(3, z3, stat_b, (z4, b1[2]))
        b4 = backward(4, z4, stat_b, b3[1])
        b = [b0, b1, b2, b3, b4]
        grad_w = wgrad_call(gx, [b0[0], b1[0], b2[0], b3[0], after(b4[0], b4[1])])
        dx = [v[2].astype(jnp.bfloat16) for v in b]
        losses = jnp.stack([stat_a[2], stat_b[2]])
        return losses, grad_w, jnp.concatenate(dx[:3]), jnp.concatenate(dx[3:])

    row_spec = P(("dp", "tp"), None)
    label_spec = P(("dp", "tp"))
    return jax.shard_map(local_step, mesh=mesh, in_specs=(row_spec, row_spec, label_spec, label_spec, P(None, "tp")), out_specs=(P("dp"), P("dp", "tp"), row_spec, row_spec), check_vma=False)
```
